32 devices in a mesh: dp: 2 (over x), row: 4 (over z), col: 4 (over y, core).
Axes of the slice: x: 2, y: 2, z: 4, core: 2. Of those that a mesh axis runs over, the one named last changes fastest.
Arguments:
- expand_gradient: bfloat16 [2, 4096, 5120], P('dp', 'row', 'col'), may hold values from -24 to 24, as said below
- expand_master: float32 [4096, 5120], P(('row', 'dp'), 'col'), may hold values from -0.12 to 0.12
- expand_rows: float32 [4096], P(('row', 'dp')), may hold values from 0.01 to 1
- expand_columns: float32 [5120], P('col'), may hold values from 0.01 to 1
- contract_gradient: bfloat16 [2, 5120, 4096], P('dp', 'row', 'col'), may hold values from -24 to 24, as said below
- contract_master: float32 [5120, 4096], P(('row', 'dp'), 'col'), may hold values from -0.12 to 0.12
- contract_rows: float32 [5120], P(('row', 'dp')), may hold values from 0.01 to 1
- contract_columns: float32 [4096], P('col'), may hold values from 0.01 to 1
- attend_gradient: bfloat16 [2, 4096, 4096], P('dp', 'row', 'col'), may hold values from -24 to 24, as said below
- attend_master: float32 [4096, 4096], P(('row', 'dp'), 'col'), may hold values from -0.12 to 0.12
- attend_rows: float32 [4096], P(('row', 'dp')), may hold values from 0.01 to 1
- attend_columns: float32 [4096], P('col'), may hold values from 0.01 to 1
Outputs:
- expand_updated: float32 [4096, 5120], P(('row', 'dp'), 'col')
- expand_weights: bfloat16 [4096, 5120], P('row', 'col')
- expand_rows_next: float32 [4096], P(('row', 'dp'))
- expand_columns_next: float32 [5120], P('col')
- expand_step: float32 [4096, 5120], P(('row', 'dp'), 'col')
- contract_updated: float32 [5120, 4096], P(('row', 'dp'), 'col')
- contract_weights: bfloat16 [5120, 4096], P('row', 'col')
- contract_rows_next: float32 [5120], P(('row', 'dp'))
- contract_columns_next: float32 [4096], P('col')
- contract_step: float32 [5120, 4096], P(('row', 'dp'), 'col')
- attend_updated: float32 [4096, 4096], P(('row', 'dp'), 'col')
- attend_weights: bfloat16 [4096, 4096], P('row', 'col')
- attend_rows_next: float32 [4096], P(('row', 'dp'))
- attend_columns_next: float32 [4096], P('col')
- attend_step: float32 [4096, 4096], P(('row', 'dp'), 'col')
The draws below stay inside these ranges and needn't reach their ends.
Inputs may be any that keep to these rules, and one draw needn't show every extreme that they name: `expand_gradient`: each replica's gradient, of any scale from entry to entry. `contract_gradient`: each replica's gradient, of any scale from entry to entry. `attend_gradient`: each replica's gradient, of any scale from entry to entry.
All inputs are finite; a program needn't handle non-finite values.
Results may differ from the reference program's by a relative error of at most 0.0004.
Values may be sent and summed in bfloat16 or wider, within the bound.
A program may use at most 128 MiB of HBM per device.

```python
import math
import jax
import jax.numpy as jnp
from jax import lax

D = 4096
FF = 5120
INNER = 4096
REPLICAS = 2


def scale_field(key, height, width):
    row_pos = jnp.arange(height, dtype=jnp.float32) / height
    col_pos = jnp.arange(width, dtype=jnp.float32) / width
    logs = jnp.zeros((height, width), jnp.float32)
    for term in range(3):
        sub = jax.random.fold_in(key, 100 + term)
        freq_keys = jax.random.split(sub, 4)
        row_freq = jax.random.randint(freq_keys[0], (), 1, 5).astype(jnp.float32)
        col_freq = jax.random.randint(freq_keys[1], (), 1, 4).astype(jnp.float32)
        row_phase = jax.random.uniform(freq_keys[2], (), jnp.float32, 0.0, 2.0 * math.pi)
        col_phase = jax.random.uniform(freq_keys[3], (), jnp.float32, 0.0, 2.0 * math.pi)
        along_rows = jnp.cos(2.0 * math.pi * row_freq * row_pos + row_phase)
        along_cols = jnp.cos(2.0 * math.pi * col_freq * col_pos + col_phase)
        logs = logs + 0.6 * along_rows[:, None] * along_cols[None, :]
    return jnp.exp(logs)


def gradient_draw(key, replicas, height, width):
    field = scale_field(jax.random.fold_in(key, 7), height, width)
    noise_key = jax.random.fold_in(key, 11)
    noise = jax.random.normal(noise_key, (replicas, height, width), jnp.float32)
    values = jnp.clip(2.0 * noise * field[None, :, :], -24.0, 24.0)
    return values.astype(jnp.bfloat16)


def draw_expand_gradient(key, part):
    return gradient_draw(jax.random.fold_in(key, 1), REPLICAS, D, FF)


def draw_contract_gradient(key, part):
    return gradient_draw(jax.random.fold_in(key, 2), REPLICAS, FF, D)


def draw_attend_gradient(key, part):
    return gradient_draw(jax.random.fold_in(key, 3), REPLICAS, INNER, D)


def level_of(rng, shape, cuts, smallest, largest):
    factor_of = 1.0
    for position, parts in cuts:
        heights = jax.random.uniform(jax.random.fold_in(jax.random.fold_in(rng, 6), position), (parts,), jnp.float32, smallest / len(cuts), largest / len(cuts))
        factor_of = factor_of * jnp.repeat(jnp.exp(heights), shape[position] // parts).reshape((-1,) + (1,) * (len(shape) - 1 - position))
    return factor_of


def bell_draw(rng, extent, spread, limit, shards=(), held_as=jnp.bfloat16):
    values = spread * jax.random.normal(rng, extent, jnp.float32)
    if shards:
        values = values * level_of(rng, extent, shards, -0.22, 0.18)
    return jnp.clip(values, -limit, limit).astype(held_as)


def setup_inputs(seed: int = 0) -> dict:
    key_of = jax.random.split(jax.random.key(seed), 13)
    expand_gradient = draw_expand_gradient(jax.random.fold_in(key_of[12], 71), 0)
    expand_master = bell_draw(key_of[1], (D, FF), 0.02, 0.12, ((0, 8), (1, 4)), jnp.float32)
    expand_rows = jnp.clip(jnp.exp(math.log(1.0) - 4.6051702 * jax.random.uniform(key_of[2], (D,), jnp.float32) ** level_of(key_of[2], (D,), ((0, 8),), -0.2, 0.2)), 0.01, 1.0)
    expand_columns = jnp.clip(jnp.exp(math.log(1.0) - 4.6051702 * jax.random.uniform(key_of[3], (FF,), jnp.float32) ** level_of(key_of[3], (FF,), ((0, 4),), -0.2, 0.2)), 0.01, 1.0)
    contract_gradient = draw_contract_gradient(jax.random.fold_in(key_of[12], 71), 0)
    contract_master = bell_draw(key_of[5], (FF, D), 0.02, 0.12, ((0, 8), (1, 4)), jnp.float32)
    contract_rows = jnp.clip(jnp.exp(math.log(1.0) - 4.6051702 * jax.random.uniform(key_of[6], (FF,), jnp.float32) ** level_of(key_of[6], (FF,), ((0, 8),), -0.2, 0.2)), 0.01, 1.0)
    contract_columns = jnp.clip(jnp.exp(math.log(1.0) - 4.6051702 * jax.random.uniform(key_of[7], (D,), jnp.float32) ** level_of(key_of[7], (D,), ((0, 4),), -0.2, 0.2)), 0.01, 1.0)
    attend_gradient = draw_attend_gradient(jax.random.fold_in(key_of[12], 71), 0)
    attend_master = bell_draw(key_of[9], (INNER, D), 0.02, 0.12, ((0, 8), (1, 4)), jnp.float32)
    attend_rows = jnp.clip(jnp.exp(math.log(1.0) - 4.6051702 * jax.random.uniform(key_of[10], (INNER,), jnp.float32) ** level_of(key_of[10], (INNER,), ((0, 8),), -0.2, 0.2)), 0.01, 1.0)
    attend_columns = jnp.clip(jnp.exp(math.log(1.0) - 4.6051702 * jax.random.uniform(key_of[11], (D,), jnp.float32) ** level_of(key_of[11], (D,), ((0, 4),), -0.2, 0.2)), 0.01, 1.0)
    return dict(expand_gradient=expand_gradient, expand_master=expand_master, expand_rows=expand_rows, expand_columns=expand_columns, contract_gradient=contract_gradient, contract_master=contract_master, contract_rows=contract_rows, contract_columns=contract_columns, attend_gradient=attend_gradient, attend_master=attend_master, attend_rows=attend_rows, attend_columns=attend_columns)


def adapt(gradient, master, row_stat, column_stat):
    total = gradient[0].astype(jnp.float32)
    for which in range(1, gradient.shape[0]):
        total = total + gradient[which].astype(jnp.float32)
    mean_grad = total / gradient.shape[0]
    squares = mean_grad * mean_grad + 1e-30
    rows_next = 0.9 * row_stat + 0.1 * lax.optimization_barrier(jnp.mean(squares, axis=1))
    columns_next = 0.9 * column_stat + 0.1 * lax.optimization_barrier(jnp.mean(squares, axis=0))
    row_mean = jnp.mean(rows_next)
    update_raw = mean_grad * jnp.sqrt(row_mean / (rows_next[:, None] * columns_next[None, :]))
    clip_scale = jnp.maximum(1.0, jnp.sqrt(jnp.mean(update_raw * update_raw)))
    step_taken = update_raw / clip_scale
    updated = master - 0.01 * step_taken
    return (updated, updated.astype(jnp.bfloat16), rows_next, columns_next, step_taken)

def reference(expand_gradient, expand_master, expand_rows, expand_columns, contract_gradient, contract_master, contract_rows, contract_columns, attend_gradient, attend_master, attend_rows, attend_columns):
    first = adapt(expand_gradient, expand_master, expand_rows, expand_columns)
    second = adapt(contract_gradient, contract_master, contract_rows, contract_columns)
    third = adapt(attend_gradient, attend_master, attend_rows, attend_columns)
    return (first[0], first[1], first[2], first[3], first[4], second[0], second[1], second[2], second[3], second[4], third[0], third[1], third[2], third[3], third[4])
```

```python
import functools
import math

import jax
import jax.numpy as jnp
from jax import lax
from jax.experimental import pallas as pl
from jax.experimental.pallas import tpu as pltpu
from jax.sharding import PartitionSpec as P

tiny_square = 1e-30
decay_rate = 0.9
learn_rate = 0.01
LANES = 128
MESH = pl.DeviceIdType.MESH
f32 = jnp.float32
bf16 = jnp.bfloat16


def chunk_count(rows):
    return 2 if rows % 64 == 0 else 1


def block_rows(rows):
    return 32 if rows % 32 == 0 else rows


def kernel(axes, shapes, *refs):
    dp_count, row_count, col_count = axes
    refs = list(refs)

    def take(count):
        taken = refs[:count]
        del refs[:count]
        return taken

    grads, masters, row_stats, col_stats = take(3), take(3), take(3), take(3)
    out_updated, out_weights, out_rows, out_cols, out_step = (take(3) for _ in range(5))
    own, recv, field, hold, weights = (take(3) for _ in range(5))
    row_part, row_wide, col_acc = take(3), take(3), take(3)
    rows_buf, cols_row_buf, cols_dp_buf = take(3), take(3), take(3)
    sum_col_buf, sum_row_buf, sum_dp_buf = take(3), take(3), take(3)
    rs_sems, ag_sems, rows_sems, cr_sems, cd_sems, sc_sems, sr_sems, sd_sems = (
        take(2) for _ in range(8)
    )
    (local_sems,) = take(1)

    me = {name: lax.axis_index(name) for name in ("dp", "row", "col")}
    size = {"dp": dp_count, "row": row_count, "col": col_count}

    def peer(axis, offset):
        return lax.rem(me[axis] + offset, size[axis])

    local_in = []
    for k in range(3):
        a = pltpu.make_async_copy(grads[k].at[me["dp"]], own[k], local_sems.at[k])
        b = pltpu.make_async_copy(masters[k], hold[k], local_sems.at[3 + k])
        a.start()
        b.start()
        local_in.append((a, b))

    barrier = pltpu.get_barrier_semaphore()
    total_peers = 0
    for axis in ("dp", "row", "col"):
        for offset in range(1, size[axis]):
            pl.semaphore_signal(
                barrier, inc=1, device_id={axis: peer(axis, offset)}, device_id_type=MESH
            )
            total_peers += 1
    pl.semaphore_wait(barrier, total_peers)

    def rows_of(k, half):
        rows = shapes[k][0]
        count = chunk_count(rows)
        if half >= count:
            return None
        return pl.ds(half * (rows // count), rows // count)

    def scatter(k, half):
        part = rows_of(k, half)
        copies = []
        if part is not None:
            for offset in range(1, dp_count):
                other = peer("dp", offset)
                copies.append(
                    pltpu.make_async_remote_copy(
                        src_ref=grads[k].at[other, part],
                        dst_ref=recv[k].at[offset - 1, part],
                        send_sem=rs_sems[0].at[k, half, offset - 1],
                        recv_sem=rs_sems[1].at[k, half, offset - 1],
                        device_id={"dp": other},
                        device_id_type=MESH,
                    )
                )
        for copy in copies:
            copy.start()
        return copies

    def gather(k, half):
        part = rows_of(k, half)
        copies = []
        if part is not None:
            for offset in range(1, dp_count):
                copies.append(
                    pltpu.make_async_remote_copy(
                        src_ref=weights[k].at[part],
                        dst_ref=out_weights[k].at[me["dp"], part],
                        send_sem=ag_sems[0].at[k, half, offset - 1],
                        recv_sem=ag_sems[1].at[k, half, offset - 1],
                        device_id={"dp": peer("dp", offset)},
                        device_id_type=MESH,
                    )
                )
        for copy in copies:
            copy.start()
        return copies

    def share(axis, buf, sems, k):
        copies = []
        for offset in range(1, size[axis]):
            copies.append(
                pltpu.make_async_remote_copy(
                    src_ref=buf.at[me[axis]],
                    dst_ref=buf.at[me[axis]],
                    send_sem=sems[0].at[k, offset - 1],
                    recv_sem=sems[1].at[k, offset - 1],
                    device_id={axis: peer(axis, offset)},
                    device_id_type=MESH,
                )
            )
        for copy in copies:
            copy.start()
        return copies

    def finish(copies):
        for copy in copies:
            copy.wait()

    def total_of(buf, axis, part=slice(None)):
        result = buf[0, part]
        for which in range(1, size[axis]):
            result = result + buf[which, part]
        return result

    def fold(block):
        result = block[0:8]
        for start in range(8, block.shape[0], 8):
            result = result + block[start : start + 8]
        return result

    def mean_pass(k, half):
        rows, width = shapes[k]
        count = chunk_count(rows)
        if half >= count:
            return
        chunk = rows // count
        step = block_rows(chunk)
        tiles = width // LANES

        def body(i, carry):
            at = pl.ds(pl.multiple_of(half * chunk + i * step, step), step)
            along = jnp.zeros((step, LANES), f32)
            new = []
            for t in range(tiles):
                lanes = pl.ds(t * LANES, LANES)
                value = own[k][at, lanes].astype(f32)
                for offset in range(dp_count - 1):
                    value = value + recv[k][offset, at, lanes].astype(f32)
                value = value * (1.0 / dp_count)
                field[k][at, lanes] = value
                square = value * value + tiny_square
                along = along + square
                new.append(carry[t] + fold(square))
            row_part[k][at, :] = along
            return tuple(new)

        if half == 0:
            init = tuple(jnp.zeros((8, LANES), f32) for _ in range(tiles))
        else:
            init = tuple(col_acc[k][:, t * LANES : (t + 1) * LANES] for t in range(tiles))
        result = lax.fori_loop(0, chunk // step, body, init)
        for t in range(tiles):
            col_acc[k][:, t * LANES : (t + 1) * LANES] = result[t]

    def stats(k):
        rows, width = shapes[k]
        padded = row_part[k].shape[0]
        if padded != rows:
            row_part[k][rows:, :] = jnp.zeros((padded - rows, LANES), f32)
        for start in range(0, padded, LANES):
            block = row_part[k][start : start + LANES, :].T
            rows_buf[k][me["col"], :, start : start + LANES] = jnp.sum(
                block, axis=0, keepdims=True
            )
        cols_row_buf[k][me["row"]] = jnp.sum(col_acc[k][...], axis=0, keepdims=True)
        first = share("col", rows_buf[k], rows_sems, k)
        second = share("row", cols_row_buf[k], cr_sems, k)
        finish(second)
        cols_dp_buf[k][me["dp"]] = total_of(cols_row_buf[k], "row")
        third = share("dp", cols_dp_buf[k], cd_sems, k)
        finish(first)
        rows_next = decay_rate * row_stats[k][...] + ((1.0 - decay_rate) / (width * col_count)) * (
            total_of(rows_buf[k], "col")
        )
        out_rows[k][...] = rows_next
        inverse = lax.rsqrt(rows_next)
        for start in range(0, padded, LANES):
            row_wide[k][start : start + LANES, :] = jnp.broadcast_to(
                inverse[:, start : start + LANES], (LANES, LANES)
            ).T
        return third

    def update_pass(k, pending):
        rows, width = shapes[k]
        height = rows * dp_count * row_count
        step = block_rows(rows)
        tiles = width // LANES
        finish(pending)
        cols_next = decay_rate * col_stats[k][...] + ((1.0 - decay_rate) / height) * total_of(
            cols_dp_buf[k], "dp"
        )
        out_cols[k][...] = cols_next
        inverse = lax.rsqrt(cols_next)

        def body(i, carry):
            at = pl.ds(pl.multiple_of(i * step, step), step)
            wide = row_wide[k][at, :]
            for t in range(tiles):
                lanes = pl.ds(t * LANES, LANES)
                value = field[k][at, lanes] * wide * inverse[:, t * LANES : (t + 1) * LANES]
                field[k][at, lanes] = value
                carry = carry + fold(value * value)
            return carry

        squares = lax.fori_loop(0, rows // step, body, jnp.zeros((8, LANES), f32))
        padded = row_part[k].shape[0]
        rows_next = out_rows[k][...]
        if padded != rows:
            lane = lax.broadcasted_iota(jnp.int32, rows_next.shape, 1)
            rows_next = jnp.where(lane < rows, rows_next, 0.0)
        row_total = rows_next[:, :LANES]
        for start in range(LANES, padded, LANES):
            row_total = row_total + rows_next[:, start : start + LANES]
        row_total = jnp.broadcast_to(row_total, (8, LANES))
        sum_col_buf[k][me["col"]] = squares
        finish(share("col", sum_col_buf[k], sc_sems, k))
        sum_row_buf[k][me["row"], 0:8] = total_of(sum_col_buf[k], "col")
        sum_row_buf[k][me["row"], 8:16] = row_total
        finish(share("row", sum_row_buf[k], sr_sems, k))
        sum_dp_buf[k][me["dp"]] = total_of(sum_row_buf[k], "row")
        return share("dp", sum_dp_buf[k], sd_sems, k)

    local_out = []

    def final_pass(k, pending):
        rows, width = shapes[k]
        height = rows * dp_count * row_count
        step = block_rows(rows)
        tiles = width // LANES
        finish(pending)
        both = total_of(sum_dp_buf[k], "dp")
        squares = jnp.sum(jnp.sum(both[0:8], axis=0, keepdims=True), axis=1, keepdims=True)
        row_mean = jnp.sum(both[8:9], axis=1, keepdims=True) / height
        mean_square = row_mean * squares / (height * width * col_count)
        clip_scale = jnp.maximum(1.0, jnp.sqrt(mean_square))
        scale = jnp.broadcast_to(jnp.sqrt(row_mean) / clip_scale, (8, LANES))
        scale = jnp.broadcast_to(scale[0:1], (step, LANES))
        local_in[k][1].wait()

        def body(i, carry):
            at = pl.ds(pl.multiple_of(i * step, step), step)
            for t in range(tiles):
                lanes = pl.ds(t * LANES, LANES)
                taken = field[k][at, lanes] * scale
                updated = hold[k][at, lanes] - learn_rate * taken
                field[k][at, lanes] = taken
                hold[k][at, lanes] = updated
                weights[k][at, lanes] = updated.astype(bf16)
            return carry

        lax.fori_loop(0, rows // step, body, 0)

    def write_out(k):
        for which, (source, target) in enumerate(
            (
                (field[k], out_step[k]),
                (hold[k], out_updated[k]),
                (weights[k], out_weights[k].at[me["dp"]]),
            )
        ):
            copy = pltpu.make_async_copy(source, target, local_sems.at[6 + 3 * which + k])
            copy.start()
            local_out.append(copy)

    order = (0, 1, 2)
    first, second, third = order
    arriving = {}
    sending = []

    def launch_scatter(k, half):
        arriving[k, half] = scatter(k, half)

    def launch_gather(k, half):
        sending.extend(gather(k, half))

    def arrive(k, half):
        if half == 0:
            local_in[k][0].wait()
        finish(arriving[k, half])
        mean_pass(k, half)

    launch_scatter(first, 0)
    launch_scatter(first, 1)
    arrive(first, 0)
    launch_scatter(second, 0)
    arrive(first, 1)
    cols_first = stats(first)
    launch_scatter(second, 1)
    arrive(second, 0)
    sums_first = update_pass(first, cols_first)
    launch_scatter(third, 0)
    arrive(second, 1)
    cols_second = stats(second)
    launch_scatter(third, 1)
    final_pass(first, sums_first)
    write_out(first)
    arrive(third, 0)
    sums_second = update_pass(second, cols_second)
    launch_gather(first, 0)
    arrive(third, 1)
    cols_third = stats(third)
    launch_gather(first, 1)
    final_pass(second, sums_second)
    write_out(second)
    sums_third = update_pass(third, cols_third)
    launch_gather(second, 0)
    final_pass(third, sums_third)
    launch_gather(second, 1)
    launch_gather(third, 0)
    launch_gather(third, 1)
    write_out(third)
    finish(sending)
    for copy in local_out:
        copy.wait()


def body(axes, *args):
    dp_count, row_count, col_count = axes
    grads, masters, row_stats, col_stats = (list(args[which::4]) for which in range(4))
    shapes = tuple(master.shape for master in masters)
    grads = [g.reshape((dp_count,) + shape) for g, shape in zip(grads, shapes)]
    padded = [-(-rows // LANES) * LANES for rows, _ in shapes]
    row_stats = [
        jnp.pad(r, (0, extra - r.shape[0]), constant_values=1.0).reshape(1, extra)
        for r, extra in zip(row_stats, padded)
    ]
    col_stats = [c.reshape(1, -1) for c in col_stats]
    anywhere = pl.BlockSpec(memory_space=pl.ANY)
    inside = pl.BlockSpec(memory_space=pltpu.VMEM)
    three = range(3)

    def vmem(make, dtype=f32):
        return [pltpu.VMEM(make(k), dtype) for k in three]

    def sems(*shape):
        return [pltpu.SemaphoreType.DMA(shape)] * 2

    scratch = (
        vmem(lambda k: shapes[k], bf16)
        + vmem(lambda k: (dp_count - 1,) + shapes[k], bf16)
        + vmem(lambda k: shapes[k])
        + vmem(lambda k: shapes[k])
        + vmem(lambda k: shapes[k], bf16)
        + vmem(lambda k: (padded[k], LANES))
        + vmem(lambda k: (padded[k], LANES))
        + vmem(lambda k: (8, shapes[k][1]))
        + vmem(lambda k: (col_count, 1, padded[k]))
        + vmem(lambda k: (row_count, 1, shapes[k][1]))
        + vmem(lambda k: (dp_count, 1, shapes[k][1]))
        + vmem(lambda k: (col_count, 8, LANES))
        + vmem(lambda k: (row_count, 16, LANES))
        + vmem(lambda k: (dp_count, 16, LANES))
        + sems(3, 2, dp_count - 1)
        + sems(3, 2, dp_count - 1)
        + sems(3, col_count - 1)
        + sems(3, row_count - 1)
        + sems(3, dp_count - 1)
        + sems(3, col_count - 1)
        + sems(3, row_count - 1)
        + sems(3, dp_count - 1)
        + [pltpu.SemaphoreType.DMA((15,))]
    )
    struct = jax.ShapeDtypeStruct
    results = pl.pallas_call(
        functools.partial(kernel, axes, shapes),
        out_shape=(
            [struct(shapes[k], f32) for k in three]
            + [struct((dp_count,) + shapes[k], bf16) for k in three]
            + [struct((1, padded[k]), f32) for k in three]
            + [struct((1, shapes[k][1]), f32) for k in three]
            + [struct(shapes[k], f32) for k in three]
        ),
        in_specs=[anywhere] * 6 + [inside] * 6,
        out_specs=[anywhere] * 6 + [inside] * 6 + [anywhere] * 3,
        scratch_shapes=scratch,
        compiler_params=pltpu.CompilerParams(
            collective_id=0, has_side_effects=True, vmem_limit_bytes=60 * 1024 * 1024
        ),
    )(*grads, *masters, *row_stats, *col_stats)
    outputs = []
    for k in three:
        updated, gathered, rows_next, cols_next, taken = results[k::3]
        outputs += [
            updated,
            gathered.reshape(-1, shapes[k][1]),
            rows_next.reshape(-1)[: shapes[k][0]],
            cols_next.reshape(-1),
            taken,
        ]
    return tuple(outputs)


def solution(mesh):
    axes = tuple(mesh.shape[name] for name in ("dp", "row", "col"))
    matrix = (P("dp", "row", "col"), P(("row", "dp"), "col"), P(("row", "dp")), P("col"))
    result = (
        P(("row", "dp"), "col"),
        P("row", "col"),
        P(("row", "dp")),
        P("col"),
        P(("row", "dp"), "col"),
    )
    return jax.shard_map(
        functools.partial(body, axes),
        mesh=mesh,
        in_specs=matrix * 3,
        out_specs=result * 3,
        check_vma=False,
    )
```

```python
import functools
import math

import jax
import jax.numpy as jnp
from jax import lax
from jax.experimental import pallas as pl
from jax.experimental.pallas import tpu as pltpu
from jax.sharding import PartitionSpec as P

tiny_square = 1e-30
decay_rate = 0.9
learn_rate = 0.01
LANES = 128
last = 2
MESH = pl.DeviceIdType.MESH
f32 = jnp.float32
bf16 = jnp.bfloat16


def chunk_count(rows):
    return 2 if rows % 64 == 0 else 1


def block_rows(rows):
    return 32 if rows % 32 == 0 else rows


def kernel(axes, shapes, *refs):
    dp_count, row_count, col_count = axes
    refs = list(refs)

    def take(count):
        taken = refs[:count]
        del refs[:count]
        return taken

    grads, masters, row_stats, col_stats = take(3), take(3), take(3), take(3)
    out_updated, out_weights, out_rows, out_cols, out_step = (take(3) for _ in range(5))
    own, recv, field, hold, weights = (take(3) for _ in range(5))
    row_part, row_wide, col_acc = take(3), take(3), take(3)
    rows_buf, cols_row_buf, cols_dp_buf = take(3), take(3), take(3)
    sum_col_buf, sum_row_buf, sum_dp_buf = take(3), take(3), take(3)
    rs_sems, ag_sems, rows_sems, cr_sems, cd_sems, sc_sems, sr_sems, sd_sems = (
        take(2) for _ in range(8)
    )
    (local_sems,) = take(1)

    me = {name: lax.axis_index(name) for name in ("dp", "row", "col")}
    size = {"dp": dp_count, "row": row_count, "col": col_count}

    def peer(axis, offset):
        return lax.rem(me[axis] + offset, size[axis])

    local_in = []
    for k in range(3):
        a = pltpu.make_async_copy(grads[k].at[me["dp"]], own[k], local_sems.at[k])
        b = pltpu.make_async_copy(masters[k], hold[k], local_sems.at[3 + k])
        a.start()
        b.start()
        local_in.append((a, b))

    barrier = pltpu.get_barrier_semaphore()
    total_peers = 0
    for axis in ("dp", "row", "col"):
        for offset in range(1, size[axis]):
            pl.semaphore_signal(
                barrier, inc=1, device_id={axis: peer(axis, offset)}, device_id_type=MESH
            )
            total_peers += 1
    pl.semaphore_wait(barrier, total_peers)

    def rows_of(k, half):
        rows = shapes[k][0]
        count = chunk_count(rows)
        if half >= count:
            return None
        return pl.ds(half * (rows // count), rows // count)

    def scatter(k, half):
        part = rows_of(k, half)
        copies = []
        if part is not None:
            for offset in range(1, dp_count):
                other = peer("dp", offset)
                copies.append(
                    pltpu.make_async_remote_copy(
                        src_ref=grads[k].at[other, part],
                        dst_ref=recv[k].at[offset - 1, part],
                        send_sem=rs_sems[0].at[k, half, offset - 1],
                        recv_sem=rs_sems[1].at[k, half, offset - 1],
                        device_id={"dp": other},
                        device_id_type=MESH,
                    )
                )
        for copy in copies:
            copy.start()
        return copies

    def gather(k, half):
        part = rows_of(k, half)
        copies = []
        if part is not None:
            for offset in range(1, dp_count):
                copies.append(
                    pltpu.make_async_remote_copy(
                        src_ref=weights[k].at[part],
                        dst_ref=out_weights[k].at[me["dp"], part],
                        send_sem=ag_sems[0].at[k, half, offset - 1],
                        recv_sem=ag_sems[1].at[k, half, offset - 1],
                        device_id={"dp": peer("dp", offset)},
                        device_id_type=MESH,
                    )
                )
        for copy in copies:
            copy.start()
        return copies

    def share(axis, buf, sems, k):
        copies = []
        for offset in range(1, size[axis]):
            copies.append(
                pltpu.make_async_remote_copy(
                    src_ref=buf.at[me[axis]],
                    dst_ref=buf.at[me[axis]],
                    send_sem=sems[0].at[k, offset - 1],
                    recv_sem=sems[1].at[k, offset - 1],
                    device_id={axis: peer(axis, offset)},
                    device_id_type=MESH,
                )
            )
        for copy in copies:
            copy.start()
        return copies

    def finish(copies):
        for copy in copies:
            copy.wait()

    def total_of(buf, axis, part=slice(None)):
        result = buf[0, part]
        for which in range(1, size[axis]):
            result = result + buf[which, part]
        return result

    def fold(block):
        result = block[0:8]
        for start in range(8, block.shape[0], 8):
            result = result + block[start : start + 8]
        return result

    def mean_pass(k, half):
        rows, width = shapes[k]
        count = chunk_count(rows)
        if half >= count:
            return
        chunk = rows // count
        step = block_rows(chunk)
        tiles = width // LANES

        def body(i, carry):
            at = pl.ds(pl.multiple_of(half * chunk + i * step, step), step)
            along = jnp.zeros((step, LANES), f32)
            new = []
            for t in range(tiles):
                lanes = pl.ds(t * LANES, LANES)
                value = own[k][at, lanes].astype(f32)
                for offset in range(dp_count - 1):
                    value = value + recv[k][offset, at, lanes].astype(f32)
                value = value * (1.0 / dp_count)
                field[k][at, lanes] = value
                square = value * value + tiny_square
                along = along + square
                new.append(carry[t] + fold(square))
            row_part[k][at, :] = along
            return tuple(new)

        if half == 0:
            init = tuple(jnp.zeros((8, LANES), f32) for _ in range(tiles))
        else:
            init = tuple(col_acc[k][:, t * LANES : (t + 1) * LANES] for t in range(tiles))
        result = lax.fori_loop(0, chunk // step, body, init)
        for t in range(tiles):
            col_acc[k][:, t * LANES : (t + 1) * LANES] = result[t]

    def stats(k):
        rows, width = shapes[k]
        padded = row_part[k].shape[0]
        if padded != rows:
            row_part[k][rows:, :] = jnp.zeros((padded - rows, LANES), f32)
        for start in range(0, padded, LANES):
            block = row_part[k][start : start + LANES, :].T
            rows_buf[k][me["col"], :, start : start + LANES] = jnp.sum(
                block, axis=0, keepdims=True
            )
        cols_row_buf[k][me["row"]] = jnp.sum(col_acc[k][...], axis=0, keepdims=True)
        first = share("col", rows_buf[k], rows_sems, k)
        second = share("row", cols_row_buf[k], cr_sems, k)
        finish(second)
        cols_dp_buf[k][me["dp"]] = total_of(cols_row_buf[k], "row")
        third = share("dp", cols_dp_buf[k], cd_sems, k)
        finish(first)
        rows_next = decay_rate * row_stats[k][...].reshape(1, -1) + ((1.0 - decay_rate) / (width * col_count)) * (
            total_of(rows_buf[k], "col")
        )
        out_rows[k][...] = rows_next
        inverse = lax.rsqrt(rows_next)
        for start in range(0, padded, LANES):
            row_wide[k][start : start + LANES, :] = jnp.broadcast_to(
                inverse[:, start : start + LANES], (LANES, LANES)
            ).T
        return third

    def update_pass(k, pending):
        rows, width = shapes[k]
        height = rows * dp_count * row_count
        step = block_rows(rows)
        tiles = width // LANES
        finish(pending)
        cols_next = decay_rate * col_stats[k][...].reshape(1, -1) + ((1.0 - decay_rate) / height) * total_of(
            cols_dp_buf[k], "dp"
        )
        out_cols[k][...] = cols_next
        inverse = lax.rsqrt(cols_next)

        def body(i, carry):
            at = pl.ds(pl.multiple_of(i * step, step), step)
            wide = row_wide[k][at, :]
            for t in range(tiles):
                lanes = pl.ds(t * LANES, LANES)
                value = field[k][at, lanes] * wide * inverse[:, t * LANES : (t + 1) * LANES]
                field[k][at, lanes] = value
                carry = carry + fold(value * value)
            return carry

        squares = lax.fori_loop(0, rows // step, body, jnp.zeros((8, LANES), f32))
        padded = row_part[k].shape[0]
        rows_next = out_rows[k][...]
        if padded != rows:
            lane = lax.broadcasted_iota(jnp.int32, rows_next.shape, 1)
            rows_next = jnp.where(lane < rows, rows_next, 0.0)
        row_total = rows_next[:, :LANES]
        for start in range(LANES, padded, LANES):
            row_total = row_total + rows_next[:, start : start + LANES]
        row_total = jnp.broadcast_to(row_total, (8, LANES))
        sum_col_buf[k][me["col"]] = squares
        finish(share("col", sum_col_buf[k], sc_sems, k))
        sum_row_buf[k][me["row"], 0:8] = total_of(sum_col_buf[k], "col")
        sum_row_buf[k][me["row"], 8:16] = row_total
        finish(share("row", sum_row_buf[k], sr_sems, k))
        sum_dp_buf[k][me["dp"]] = total_of(sum_row_buf[k], "row")
        return share("dp", sum_dp_buf[k], sd_sems, k)

    local_out = []

    def final_pass(k, pending):
        rows, width = shapes[k]
        height = rows * dp_count * row_count
        step = block_rows(rows)
        tiles = width // LANES
        finish(pending)
        both = total_of(sum_dp_buf[k], "dp")
        squares = jnp.sum(jnp.sum(both[0:8], axis=0, keepdims=True), axis=1, keepdims=True)
        row_mean = jnp.sum(both[8:9], axis=1, keepdims=True) / height
        mean_square = row_mean * squares / (height * width * col_count)
        clip_scale = jnp.maximum(1.0, jnp.sqrt(mean_square))
        scale = jnp.broadcast_to(jnp.sqrt(row_mean) / clip_scale, (8, LANES))
        scale = jnp.broadcast_to(scale[0:1], (step, LANES))
        local_in[k][1].wait()

        def body(i, carry):
            at = pl.ds(pl.multiple_of(i * step, step), step)
            for t in range(tiles):
                lanes = pl.ds(t * LANES, LANES)
                taken = field[k][at, lanes] * scale
                updated = hold[k][at, lanes] - learn_rate * taken
                field[k][at, lanes] = taken
                hold[k][at, lanes] = updated
                weights[k][at, lanes] = updated.astype(bf16)
            return carry

        lax.fori_loop(0, rows // step, body, 0)

    def write_out(k):
        for which, (source, target) in enumerate(
            (
                (field[k], out_step[k]),
                (hold[k], out_updated[k]),
                (weights[k], out_weights[k] if k == last else out_weights[k].at[me["dp"]]),
            )
        ):
            copy = pltpu.make_async_copy(source, target, local_sems.at[6 + 3 * which + k])
            copy.start()
            local_out.append(copy)

    first, second, third = 0, 1, last
    arriving = {}
    sending = []

    def launch_scatter(k, half):
        arriving[k, half] = scatter(k, half)

    def launch_gather(k, half):
        sending.extend(gather(k, half))

    def arrive(k, half):
        if half == 0:
            local_in[k][0].wait()
        finish(arriving[k, half])
        mean_pass(k, half)

    launch_scatter(first, 0)
    launch_scatter(first, 1)
    arrive(first, 0)
    launch_scatter(second, 0)
    arrive(first, 1)
    cols_first = stats(first)
    launch_scatter(second, 1)
    arrive(second, 0)
    sums_first = update_pass(first, cols_first)
    launch_scatter(third, 0)
    arrive(second, 1)
    cols_second = stats(second)
    launch_scatter(third, 1)
    final_pass(first, sums_first)
    write_out(first)
    arrive(third, 0)
    sums_second = update_pass(second, cols_second)
    launch_gather(first, 0)
    arrive(third, 1)
    cols_third = stats(third)
    launch_gather(first, 1)
    final_pass(second, sums_second)
    write_out(second)
    sums_third = update_pass(third, cols_third)
    launch_gather(second, 0)
    final_pass(third, sums_third)
    launch_gather(second, 1)
    write_out(third)
    finish(sending)
    for copy in local_out:
        copy.wait()


def write_results(*refs):
    small_in, large_in = refs[0:6], refs[6:15]
    small_out, large_out = refs[15:21], list(refs[21:30])
    held, (in_sems, out_sems) = refs[30:39], refs[39:41]
    large_out[3 + last] = large_out[3 + last].at[lax.axis_index("dp")]
    reads = [
        pltpu.make_async_copy(large_in[i], held[i], in_sems.at[i]) for i in range(len(held))
    ]
    writes = [
        pltpu.make_async_copy(held[i], large_out[i], out_sems.at[i]) for i in range(len(held))
    ]
    for copy in reads:
        copy.start()
    for source, target in zip(small_in, small_out):
        target[...] = source[0, :]
    for read, write in zip(reads, writes):
        read.wait()
        write.start()
    for copy in writes:
        copy.wait()


def body(axes, *args):
    dp_count, row_count, col_count = axes
    grads, masters, row_stats, col_stats = (list(args[which::4]) for which in range(4))
    shapes = tuple(master.shape for master in masters)
    grads = [g.reshape((dp_count,) + shape) for g, shape in zip(grads, shapes)]
    padded = [-(-rows // LANES) * LANES for rows, _ in shapes]
    row_stats = [
        jnp.pad(r, (0, extra - r.shape[0]), constant_values=1.0)
        for r, extra in zip(row_stats, padded)
    ]
    anywhere = pl.BlockSpec(memory_space=pl.ANY)
    inside = pl.BlockSpec(memory_space=pltpu.VMEM)
    three = range(3)

    def vmem(make, dtype=f32):
        return [pltpu.VMEM(make(k), dtype) for k in three]

    def sems(*shape):
        return [pltpu.SemaphoreType.DMA(shape)] * 2

    scratch = (
        vmem(lambda k: shapes[k], bf16)
        + vmem(lambda k: (dp_count - 1,) + shapes[k], bf16)
        + vmem(lambda k: shapes[k])
        + vmem(lambda k: shapes[k])
        + vmem(lambda k: shapes[k], bf16)
        + vmem(lambda k: (padded[k], LANES))
        + vmem(lambda k: (padded[k], LANES))
        + vmem(lambda k: (8, shapes[k][1]))
        + vmem(lambda k: (col_count, 1, padded[k]))
        + vmem(lambda k: (row_count, 1, shapes[k][1]))
        + vmem(lambda k: (dp_count, 1, shapes[k][1]))
        + vmem(lambda k: (col_count, 8, LANES))
        + vmem(lambda k: (row_count, 16, LANES))
        + vmem(lambda k: (dp_count, 16, LANES))
        + sems(3, 2, dp_count - 1)
        + sems(3, 2, dp_count - 1)
        + sems(3, col_count - 1)
        + sems(3, row_count - 1)
        + sems(3, dp_count - 1)
        + sems(3, col_count - 1)
        + sems(3, row_count - 1)
        + sems(3, dp_count - 1)
        + [pltpu.SemaphoreType.DMA((15,))]
    )
    struct = jax.ShapeDtypeStruct
    results = pl.pallas_call(
        functools.partial(kernel, axes, shapes),
        out_shape=(
            [struct(shapes[k], f32) for k in three]
            + [struct(shapes[k] if k == last else (dp_count,) + shapes[k], bf16) for k in three]
            + [struct((1, padded[k]), f32) for k in three]
            + [struct((1, shapes[k][1]), f32) for k in three]
            + [struct(shapes[k], f32) for k in three]
        ),
        in_specs=[anywhere] * 6 + [inside] * 6,
        out_specs=[anywhere] * 6 + [inside] * 6 + [anywhere] * 3,
        scratch_shapes=scratch,
        compiler_params=pltpu.CompilerParams(
            collective_id=0, has_side_effects=True, vmem_limit_bytes=60 * 1024 * 1024
        ),
    )(*grads, *masters, *row_stats, *col_stats)
    smalls = list(results[6:12])
    larges = list(results[0:6]) + list(results[12:15])
    mine = results[3 + last]
    received = [
        lax.ppermute(
            mine, "dp", [(source, (source + offset) % dp_count) for source in range(dp_count)]
        )
        for offset in range(1, dp_count)
    ]
    moved = 2 * sum(large.size * large.dtype.itemsize for large in larges)
    written = pl.pallas_call(
        write_results,
        out_shape=(
            [struct(small.shape[1:], f32) for small in smalls]
            + [
                struct((dp_count,) + large.shape if which == 3 + last else large.shape, large.dtype)
                for which, large in enumerate(larges)
            ]
        ),
        in_specs=[inside] * 6 + [anywhere] * 9,
        out_specs=[inside] * 6 + [anywhere] * 9,
        scratch_shapes=[pltpu.VMEM(large.shape, large.dtype) for large in larges]
        + [pltpu.SemaphoreType.DMA((9,))] * 2,
        compiler_params=pltpu.CompilerParams(vmem_limit_bytes=60 * 1024 * 1024),
        cost_estimate=pl.CostEstimate(flops=0, bytes_accessed=moved, transcendentals=0),
    )(*smalls, *larges)
    gathered = list(written[9:12])
    me = lax.axis_index("dp")
    for offset in range(1, dp_count):
        source = lax.rem(me + dp_count - offset, dp_count)
        gathered[last] = lax.dynamic_update_index_in_dim(
            gathered[last], received[offset - 1], source, 0
        )
    outputs = []
    for k in three:
        outputs += [
            written[6 + k],
            gathered[k].reshape(-1, shapes[k][1]),
            written[k][: shapes[k][0]],
            written[3 + k],
            written[12 + k],
        ]
    return tuple(outputs)


def solution(mesh):
    axes = tuple(mesh.shape[name] for name in ("dp", "row", "col"))
    matrix = (P("dp", "row", "col"), P(("row", "dp"), "col"), P(("row", "dp")), P("col"))
    result = (
        P(("row", "dp"), "col"),
        P("row", "col"),
        P(("row", "dp")),
        P("col"),
        P(("row", "dp"), "col"),
    )
    return jax.shard_map(
        functools.partial(body, axes),
        mesh=mesh,
        in_specs=matrix * 3,
        out_specs=result * 3,
        check_vma=False,
    )
```

```python
import functools
import math

import jax
import jax.numpy as jnp
from jax import lax
from jax.experimental import pallas as pl
from jax.experimental.pallas import tpu as pltpu
from jax.sharding import PartitionSpec as P

tiny_square = 1e-30
decay_rate = 0.9
learn_rate = 0.01
LANES = 128
last = 2
MESH = pl.DeviceIdType.MESH
f32 = jnp.float32
bf16 = jnp.bfloat16


def chunk_count(rows):
    return 2 if rows % 64 == 0 else 1


def block_rows(rows):
    return 32 if rows % 32 == 0 else rows


def kernel(axes, shapes, *refs):
    dp_count, row_count, col_count = axes
    refs = list(refs)

    def take(count):
        taken = refs[:count]
        del refs[:count]
        return taken

    grads, masters, row_stats, col_stats = take(3), take(3), take(3), take(3)
    out_updated, out_weights, out_rows, out_cols, out_step = (take(3) for _ in range(5))
    own, recv, field, hold, weights = (take(3) for _ in range(5))
    row_part, row_wide, col_acc = take(3), take(3), take(3)
    rows_buf, cols_row_buf, cols_dp_buf = take(3), take(3), take(3)
    sum_col_buf, sum_row_buf, sum_dp_buf = take(3), take(3), take(3)
    rs_sems, ag_sems, rows_sems, cr_sems, cd_sems, sc_sems, sr_sems, sd_sems = (
        take(2) for _ in range(8)
    )
    (local_sems,) = take(1)

    me = {name: lax.axis_index(name) for name in ("dp", "row", "col")}
    size = {"dp": dp_count, "row": row_count, "col": col_count}

    def peer(axis, offset):
        return lax.rem(me[axis] + offset, size[axis])

    local_in = []
    for k in range(3):
        a = pltpu.make_async_copy(grads[k].at[me["dp"]], own[k], local_sems.at[k])
        b = pltpu.make_async_copy(masters[k], hold[k], local_sems.at[3 + k])
        a.start()
        b.start()
        local_in.append((a, b))

    barrier = pltpu.get_barrier_semaphore()
    total_peers = 0
    for axis in ("dp", "row", "col"):
        for offset in range(1, size[axis]):
            pl.semaphore_signal(
                barrier, inc=1, device_id={axis: peer(axis, offset)}, device_id_type=MESH
            )
            total_peers += 1
    pl.semaphore_wait(barrier, total_peers)

    def rows_of(k, half):
        rows = shapes[k][0]
        count = chunk_count(rows)
        if half >= count:
            return None
        return pl.ds(half * (rows // count), rows // count)

    def scatter(k, half):
        part = rows_of(k, half)
        copies = []
        if part is not None:
            for offset in range(1, dp_count):
                other = peer("dp", offset)
                copies.append(
                    pltpu.make_async_remote_copy(
                        src_ref=grads[k].at[other, part],
                        dst_ref=recv[k].at[offset - 1, part],
                        send_sem=rs_sems[0].at[k, half, offset - 1],
                        recv_sem=rs_sems[1].at[k, half, offset - 1],
                        device_id={"dp": other},
                        device_id_type=MESH,
                    )
                )
        for copy in copies:
            copy.start()
        return copies

    def gather(k, half):
        part = pl.ds(0, shapes[k][0]) if half is None else rows_of(k, half)
        copies = []
        if part is not None:
            for offset in range(1, dp_count):
                copies.append(
                    pltpu.make_async_remote_copy(
                        src_ref=weights[k].at[part],
                        dst_ref=out_weights[k].at[me["dp"], part],
                        send_sem=ag_sems[0].at[k, half or 0, offset - 1],
                        recv_sem=ag_sems[1].at[k, half or 0, offset - 1],
                        device_id={"dp": peer("dp", offset)},
                        device_id_type=MESH,
                    )
                )
        for copy in copies:
            copy.start()
        return copies

    def share(axis, buf, sems, k):
        copies = []
        for offset in range(1, size[axis]):
            copies.append(
                pltpu.make_async_remote_copy(
                    src_ref=buf.at[me[axis]],
                    dst_ref=buf.at[me[axis]],
                    send_sem=sems[0].at[k, offset - 1],
                    recv_sem=sems[1].at[k, offset - 1],
                    device_id={axis: peer(axis, offset)},
                    device_id_type=MESH,
                )
            )
        for copy in copies:
            copy.start()
        return copies

    def finish(copies):
        for copy in copies:
            copy.wait()

    def total_of(buf, axis, part=slice(None)):
        result = buf[0, part]
        for which in range(1, size[axis]):
            result = result + buf[which, part]
        return result

    def fold(block):
        result = block[0:8]
        for start in range(8, block.shape[0], 8):
            result = result + block[start : start + 8]
        return result

    def mean_pass(k, half):
        rows, width = shapes[k]
        count = chunk_count(rows)
        if half >= count:
            return
        chunk = rows // count
        step = block_rows(chunk)
        tiles = width // LANES

        def body(i, carry):
            at = pl.ds(pl.multiple_of(half * chunk + i * step, step), step)
            along = jnp.zeros((step, LANES), f32)
            new = []
            for t in range(tiles):
                lanes = pl.ds(t * LANES, LANES)
                value = own[k][at, lanes].astype(f32)
                for offset in range(dp_count - 1):
                    value = value + recv[k][offset, at, lanes].astype(f32)
                value = value * (1.0 / dp_count)
                field[k][at, lanes] = value
                square = value * value + tiny_square
                along = along + square
                new.append(carry[t] + fold(square))
            row_part[k][at, :] = along
            return tuple(new)

        if half == 0:
            init = tuple(jnp.zeros((8, LANES), f32) for _ in range(tiles))
        else:
            init = tuple(col_acc[k][:, t * LANES : (t + 1) * LANES] for t in range(tiles))
        result = lax.fori_loop(0, chunk // step, body, init)
        for t in range(tiles):
            col_acc[k][:, t * LANES : (t + 1) * LANES] = result[t]

    def stats(k):
        rows, width = shapes[k]
        padded = row_part[k].shape[0]
        if padded != rows:
            row_part[k][rows:, :] = jnp.zeros((padded - rows, LANES), f32)
        for start in range(0, padded, LANES):
            block = row_part[k][start : start + LANES, :].T
            rows_buf[k][me["col"], :, start : start + LANES] = jnp.sum(
                block, axis=0, keepdims=True
            )
        cols_row_buf[k][me["row"]] = jnp.sum(col_acc[k][...], axis=0, keepdims=True)
        first = share("col", rows_buf[k], rows_sems, k)
        second = share("row", cols_row_buf[k], cr_sems, k)
        finish(second)
        cols_dp_buf[k][me["dp"]] = total_of(cols_row_buf[k], "row")
        third = share("dp", cols_dp_buf[k], cd_sems, k)
        finish(first)
        rows_next = decay_rate * row_stats[k][...].reshape(1, -1) + ((1.0 - decay_rate) / (width * col_count)) * (
            total_of(rows_buf[k], "col")
        )
        out_rows[k][...] = rows_next
        inverse = lax.rsqrt(rows_next)
        for start in range(0, padded, LANES):
            row_wide[k][start : start + LANES, :] = jnp.broadcast_to(
                inverse[:, start : start + LANES], (LANES, LANES)
            ).T
        return third

    def update_pass(k, pending):
        rows, width = shapes[k]
        height = rows * dp_count * row_count
        step = block_rows(rows)
        tiles = width // LANES
        finish(pending)
        cols_next = decay_rate * col_stats[k][...].reshape(1, -1) + ((1.0 - decay_rate) / height) * total_of(
            cols_dp_buf[k], "dp"
        )
        out_cols[k][...] = cols_next
        inverse = lax.rsqrt(cols_next)

        def body(i, carry):
            at = pl.ds(pl.multiple_of(i * step, step), step)
            wide = row_wide[k][at, :]
            for t in range(tiles):
                lanes = pl.ds(t * LANES, LANES)
                value = field[k][at, lanes] * wide * inverse[:, t * LANES : (t + 1) * LANES]
                field[k][at, lanes] = value
                carry = carry + fold(value * value)
            return carry

        squares = lax.fori_loop(0, rows // step, body, jnp.zeros((8, LANES), f32))
        padded = row_part[k].shape[0]
        rows_next = out_rows[k][...]
        if padded != rows:
            lane = lax.broadcasted_iota(jnp.int32, rows_next.shape, 1)
            rows_next = jnp.where(lane < rows, rows_next, 0.0)
        row_total = rows_next[:, :LANES]
        for start in range(LANES, padded, LANES):
            row_total = row_total + rows_next[:, start : start + LANES]
        row_total = jnp.broadcast_to(row_total, (8, LANES))
        sum_col_buf[k][me["col"]] = squares
        finish(share("col", sum_col_buf[k], sc_sems, k))
        sum_row_buf[k][me["row"], 0:8] = total_of(sum_col_buf[k], "col")
        sum_row_buf[k][me["row"], 8:16] = row_total
        finish(share("row", sum_row_buf[k], sr_sems, k))
        sum_dp_buf[k][me["dp"]] = total_of(sum_row_buf[k], "row")
        return share("dp", sum_dp_buf[k], sd_sems, k)

    local_out = []

    def final_pass(k, pending):
        rows, width = shapes[k]
        height = rows * dp_count * row_count
        step = block_rows(rows)
        tiles = width // LANES
        finish(pending)
        both = total_of(sum_dp_buf[k], "dp")
        squares = jnp.sum(jnp.sum(both[0:8], axis=0, keepdims=True), axis=1, keepdims=True)
        row_mean = jnp.sum(both[8:9], axis=1, keepdims=True) / height
        mean_square = row_mean * squares / (height * width * col_count)
        clip_scale = jnp.maximum(1.0, jnp.sqrt(mean_square))
        scale = jnp.broadcast_to(jnp.sqrt(row_mean) / clip_scale, (8, LANES))
        scale = jnp.broadcast_to(scale[0:1], (step, LANES))
        local_in[k][1].wait()

        def body(i, carry):
            at = pl.ds(pl.multiple_of(i * step, step), step)
            for t in range(tiles):
                lanes = pl.ds(t * LANES, LANES)
                taken = field[k][at, lanes] * scale
                updated = hold[k][at, lanes] - learn_rate * taken
                field[k][at, lanes] = taken
                hold[k][at, lanes] = updated
                weights[k][at, lanes] = updated.astype(bf16)
            return carry

        lax.fori_loop(0, rows // step, body, 0)

    def write_out(k):
        for which, (source, target) in enumerate(
            (
                (field[k], out_step[k]),
                (hold[k], out_updated[k]),
                (weights[k], out_weights[k] if k == last else out_weights[k].at[me["dp"]]),
            )
        ):
            copy = pltpu.make_async_copy(source, target, local_sems.at[6 + 3 * which + k])
            copy.start()
            local_out.append(copy)

    first, second, third = 0, 1, last
    arriving = {}
    sending = []

    def launch_scatter(k, half):
        arriving[k, half] = scatter(k, half)

    def launch_gather(k, half):
        sending.extend(gather(k, half))

    def arrive(k, half):
        if half == 0:
            local_in[k][0].wait()
        finish(arriving[k, half])
        mean_pass(k, half)

    launch_scatter(first, 0)
    launch_scatter(first, 1)
    arrive(first, 0)
    launch_scatter(second, 0)
    arrive(first, 1)
    cols_first = stats(first)
    launch_scatter(second, 1)
    arrive(second, 0)
    sums_first = update_pass(first, cols_first)
    launch_scatter(third, 0)
    arrive(second, 1)
    cols_second = stats(second)
    launch_scatter(third, 1)
    final_pass(first, sums_first)
    write_out(first)
    arrive(third, 0)
    sums_second = update_pass(second, cols_second)
    launch_gather(first, 0)
    arrive(third, 1)
    cols_third = stats(third)
    launch_gather(first, 1)
    final_pass(second, sums_second)
    write_out(second)
    sums_third = update_pass(third, cols_third)
    launch_gather(second, None)
    final_pass(third, sums_third)
    write_out(third)
    finish(sending)
    for copy in local_out:
        copy.wait()


def write_results(*refs):
    small_in, large_in = refs[0:6], refs[6:15]
    small_out, large_out = refs[15:21], list(refs[21:30])
    held, (in_sems, out_sems) = refs[30:39], refs[39:41]
    large_out[3 + last] = large_out[3 + last].at[lax.axis_index("dp")]
    reads = [
        pltpu.make_async_copy(large_in[i], held[i], in_sems.at[i]) for i in range(len(held))
    ]
    writes = [
        pltpu.make_async_copy(held[i], large_out[i], out_sems.at[i]) for i in range(len(held))
    ]
    for copy in reads:
        copy.start()
    for source, target in zip(small_in, small_out):
        target[...] = source[0, :]
    for read, write in zip(reads, writes):
        read.wait()
        write.start()
    for copy in writes:
        copy.wait()


def body(axes, *args):
    dp_count, row_count, col_count = axes
    grads, masters, row_stats, col_stats = (list(args[which::4]) for which in range(4))
    shapes = tuple(master.shape for master in masters)
    grads = [g.reshape((dp_count,) + shape) for g, shape in zip(grads, shapes)]
    padded = [-(-rows // LANES) * LANES for rows, _ in shapes]
    row_stats = [
        jnp.pad(r, (0, extra - r.shape[0]), constant_values=1.0)
        for r, extra in zip(row_stats, padded)
    ]
    anywhere = pl.BlockSpec(memory_space=pl.ANY)
    inside = pl.BlockSpec(memory_space=pltpu.VMEM)
    three = range(3)

    def vmem(make, dtype=f32):
        return [pltpu.VMEM(make(k), dtype) for k in three]

    def sems(*shape):
        return [pltpu.SemaphoreType.DMA(shape)] * 2

    scratch = (
        vmem(lambda k: shapes[k], bf16)
        + vmem(lambda k: (dp_count - 1,) + shapes[k], bf16)
        + vmem(lambda k: shapes[k])
        + vmem(lambda k: shapes[k])
        + vmem(lambda k: shapes[k], bf16)
        + vmem(lambda k: (padded[k], LANES))
        + vmem(lambda k: (padded[k], LANES))
        + vmem(lambda k: (8, shapes[k][1]))
        + vmem(lambda k: (col_count, 1, padded[k]))
        + vmem(lambda k: (row_count, 1, shapes[k][1]))
        + vmem(lambda k: (dp_count, 1, shapes[k][1]))
        + vmem(lambda k: (col_count, 8, LANES))
        + vmem(lambda k: (row_count, 16, LANES))
        + vmem(lambda k: (dp_count, 16, LANES))
        + sems(3, 2, dp_count - 1)
        + sems(3, 2, dp_count - 1)
        + sems(3, col_count - 1)
        + sems(3, row_count - 1)
        + sems(3, dp_count - 1)
        + sems(3, col_count - 1)
        + sems(3, row_count - 1)
        + sems(3, dp_count - 1)
        + [pltpu.SemaphoreType.DMA((15,))]
    )
    struct = jax.ShapeDtypeStruct
    results = pl.pallas_call(
        functools.partial(kernel, axes, shapes),
        out_shape=(
            [struct(shapes[k], f32) for k in three]
            + [struct(shapes[k] if k == last else (dp_count,) + shapes[k], bf16) for k in three]
            + [struct((1, padded[k]), f32) for k in three]
            + [struct((1, shapes[k][1]), f32) for k in three]
            + [struct(shapes[k], f32) for k in three]
        ),
        in_specs=[anywhere] * 6 + [inside] * 6,
        out_specs=[anywhere] * 6 + [inside] * 6 + [anywhere] * 3,
        scratch_shapes=scratch,
        compiler_params=pltpu.CompilerParams(
            collective_id=0, has_side_effects=True, vmem_limit_bytes=60 * 1024 * 1024
        ),
    )(*grads, *masters, *row_stats, *col_stats)
    smalls = list(results[6:12])
    larges = list(results[0:6]) + list(results[12:15])
    mine = results[3 + last]
    received = [
        lax.ppermute(
            mine, "dp", [(source, (source + offset) % dp_count) for source in range(dp_count)]
        )
        for offset in range(1, dp_count)
    ]
    moved = 2 * sum(large.size * large.dtype.itemsize for large in larges)
    written = pl.pallas_call(
        write_results,
        out_shape=(
            [struct(small.shape[1:], f32) for small in smalls]
            + [
                struct((dp_count,) + large.shape if which == 3 + last else large.shape, large.dtype)
                for which, large in enumerate(larges)
            ]
        ),
        in_specs=[inside] * 6 + [anywhere] * 9,
        out_specs=[inside] * 6 + [anywhere] * 9,
        scratch_shapes=[pltpu.VMEM(large.shape, large.dtype) for large in larges]
        + [pltpu.SemaphoreType.DMA((9,))] * 2,
        compiler_params=pltpu.CompilerParams(vmem_limit_bytes=60 * 1024 * 1024),
        cost_estimate=pl.CostEstimate(flops=0, bytes_accessed=moved, transcendentals=0),
    )(*smalls, *larges)
    gathered = list(written[9:12])
    me = lax.axis_index("dp")
    for offset in range(1, dp_count):
        source = lax.rem(me + dp_count - offset, dp_count)
        gathered[last] = lax.dynamic_update_index_in_dim(
            gathered[last], received[offset - 1], source, 0
        )
    outputs = []
    for k in three:
        outputs += [
            written[6 + k],
            gathered[k].reshape(-1, shapes[k][1]),
            written[k][: shapes[k][0]],
            written[3 + k],
            written[12 + k],
        ]
    return tuple(outputs)


def solution(mesh):
    axes = tuple(mesh.shape[name] for name in ("dp", "row", "col"))
    matrix = (P("dp", "row", "col"), P(("row", "dp"), "col"), P(("row", "dp")), P("col"))
    result = (
        P(("row", "dp"), "col"),
        P("row", "col"),
        P(("row", "dp")),
        P("col"),
        P(("row", "dp"), "col"),
    )
    return jax.shard_map(
        functools.partial(body, axes),
        mesh=mesh,
        in_specs=matrix * 3,
        out_specs=result * 3,
        check_vma=False,
    )
```
